32 devices in a mesh: px: 8 (over y, x, core), py: 4 (over z).
Axes of the slice: x: 2, y: 2, z: 4, core: 2. Of those that a mesh axis runs over, the one named last changes fastest.
Arguments:
- cell_ids: int32 [8, 2560, 128], P('px', 'py'), may hold values from 0 to 262143, as said below
- offset_x: bfloat16 [8, 2560, 128], P('px', 'py'), may hold values from 0 to 1
- offset_y: bfloat16 [8, 2560, 128], P('px', 'py'), may hold values from 0 to 1
- mass: bfloat16 [8, 2560, 128], P('px', 'py'), may hold values from 0.25 to 4
- live: int32 [8, 2560, 128], P('px', 'py'), may hold values from 0 to 1, as said below
- tile_owner: int32 [8, 2560], P('px', 'py'), may hold values from 0 to 7, as said below
- counts: int32 [8, 4, 64], P('px', 'py'), may hold values from 0 to 30720, as said below
Outputs:
- spectrum: float32 [2, 8, 1024, 1024], P(None, None, ('px', 'py'))
- bucket_start: int32 [8, 4, 64], P('px', 'py')
The draws below stay inside these ranges and needn't reach their ends.
Inputs may be any that keep to these rules, and one draw needn't show every extreme that they name: A device's tiles stand in order of bucket, bucket = tile_owner * 8 + plane. One device has at most 240 tiles of one owner; in every draw, in each column of py, one owner has exactly 240 tiles on every device of that column. `cell_ids`: cell = (plane * 128 + row) * 256 + column, with row inside the owner's block of rows and column inside the device's block of columns; all slots of a tile, padded ones too, carry the tile's plane. In a tile the live particles come first; only the last tile of a bucket on a device has padded slots. counts[i, j, b] is the number of live particles in the tiles of bucket b on device (i, j); in every draw some bucket of every device holds 30720.
All inputs are finite; a program needn't handle non-finite values.
Results may differ from the reference program's by a relative error of at most 0.0003.
The reference program's roundings to bfloat16 on the way (of `weights`, `weight_x` and `weight_y`) count: a program that leaves them out, or rounds other values in their place, can miss the bound.
Values may be sent and summed in bfloat16 or wider, within the bound.
A program may use at most 192 MiB of HBM per device.

```python
import math
import jax
import jax.numpy as jnp
from jax import lax

NX = 1024
NY = 1024
PLANES = 8
TILE = 128
TILES_DEV = 640
RX = 128
RY = 256
CAP = 240
BUCKETS = 64
N_PX = 8
N_PY = 4


def tile_layout(key):
    base_key = jax.random.fold_in(key, 7001)
    key_hot, key_jitter, key_plane, key_fill = jax.random.split(base_key, 4)
    hot_owner = jax.random.randint(key_hot, (N_PY,), 0, N_PX)
    owner_ids = jnp.arange(N_PX, dtype=jnp.int32)
    is_hot = jnp.broadcast_to(owner_ids[None, None, :] == hot_owner[None, :, None], (N_PX, N_PY, N_PX))
    jitter = jax.random.randint(key_jitter, (N_PX, N_PY, N_PX), 1, 3)
    weights = jnp.where(is_hot, 0, (N_PX - 1 + 2 * owner_ids)[None, None, :] * jitter)
    remain = TILES_DEV - CAP
    shares = remain * weights // jnp.sum(weights, axis=-1, keepdims=True)
    leftover = remain - jnp.sum(shares, axis=-1, keepdims=True)
    order_rank = jnp.cumsum(jnp.where(is_hot, 0, 1), axis=-1) - 1
    shares = shares + jnp.where(jnp.logical_not(is_hot) & (order_rank < leftover), 1, 0)
    run_length = jnp.where(is_hot, CAP, shares)
    run_end = jnp.cumsum(run_length, axis=-1)
    tile_index = jnp.arange(TILES_DEV, dtype=jnp.int32)
    owner_of = jnp.sum((tile_index[None, None, :, None] >= run_end[:, :, None, :]).astype(jnp.int32), axis=-1)
    hot_of = jnp.broadcast_to(hot_owner[None, :, None], (N_PX, N_PY, TILES_DEV))
    tile_is_hot = owner_of == hot_of
    plane_draw = jax.random.randint(key_plane, (N_PX, N_PY, TILES_DEV), 0, PLANES)
    plane_draw = jnp.where(tile_is_hot, 0, plane_draw)
    sort_key = jnp.sort((owner_of * PLANES + plane_draw).astype(jnp.int32), axis=-1)
    closing = jnp.full((N_PX, N_PY, 1), -1, jnp.int32)
    is_last = sort_key != jnp.concatenate([sort_key[..., 1:], closing], axis=-1)
    sorted_hot = sort_key // PLANES == hot_of
    fill_count = jax.random.randint(key_fill, (N_PX, N_PY, TILES_DEV), 1, TILE + 1)
    live_count = jnp.where(is_last & jnp.logical_not(sorted_hot), fill_count, TILE)
    return (sort_key, live_count)


def bucket_tally(keys_row, live_row):
    return jax.ops.segment_sum(live_row, keys_row, num_segments=BUCKETS)


def draw_tile_owner(key, part):
    sort_key, live_count = tile_layout(key)
    return (sort_key // PLANES).reshape(N_PX, N_PY * TILES_DEV).astype(jnp.int32)


def draw_live(key, part):
    sort_key, live_count = tile_layout(key)
    slot_index = jnp.arange(TILE, dtype=jnp.int32)
    flags = (slot_index[None, None, None, :] < live_count[..., None]).astype(jnp.int32)
    return flags.reshape(N_PX, N_PY * TILES_DEV, TILE)


def draw_counts(key, part):
    sort_key, live_count = tile_layout(key)
    bucket_sums = jax.vmap(bucket_tally)(sort_key.reshape(-1, TILES_DEV), live_count.reshape(-1, TILES_DEV))
    return bucket_sums.reshape(N_PX, N_PY, BUCKETS).astype(jnp.int32)


def draw_cell_ids(key, part):
    sort_key, live_count = tile_layout(key)
    plane_ids = sort_key % PLANES
    key_x, key_y = jax.random.split(jax.random.fold_in(key, 7002))
    local_x = jax.random.randint(key_x, (N_PX, N_PY, TILES_DEV, TILE), 0, RX)
    local_y = jax.random.randint(key_y, (N_PX, N_PY, TILES_DEV, TILE), 0, RY)
    cells_all = (plane_ids[..., None] * RX + local_x) * RY + local_y
    return cells_all.reshape(N_PX, N_PY * TILES_DEV, TILE).astype(jnp.int32)


def steps_of(stream_key, shape, cuts, low, top_value):
    def one(dim, shards_of):
        steps = jax.random.uniform(jax.random.fold_in(jax.random.fold_in(stream_key, 6), dim), (shards_of,), jnp.float32, low / len(cuts), top_value / len(cuts))
        return jnp.repeat(jnp.exp(steps), shape[dim] // shards_of).reshape((-1,) + (1,) * (len(shape) - dim - 1))

    factor_of = one(*cuts[0])
    for cut in cuts[1:]:
        factor_of = factor_of * one(*cut)
    return factor_of


def setup_inputs(seed: int = 0) -> dict:
    keys = jax.random.split(jax.random.key(seed), 8)
    return {
        "cell_ids": draw_cell_ids(jax.random.fold_in(keys[7], 71), 0),
        "offset_x": jnp.clip(1.0 * jax.random.uniform(keys[1], (N_PX, N_PY * TILES_DEV, TILE), jnp.float32) ** steps_of(keys[1], (N_PX, N_PY * TILES_DEV, TILE), ((0, 8), (1, 4)), -0.2, 0.2), 0.0, 1.0).astype(jnp.bfloat16),
        "offset_y": jnp.clip(1.0 * jax.random.uniform(keys[2], (N_PX, N_PY * TILES_DEV, TILE), jnp.float32) ** steps_of(keys[2], (N_PX, N_PY * TILES_DEV, TILE), ((0, 8), (1, 4)), -0.2, 0.2), 0.0, 1.0).astype(jnp.bfloat16),
        "mass": jnp.clip(jnp.exp(math.log(4.0) - 2.7725887 * jax.random.uniform(keys[3], (N_PX, N_PY * TILES_DEV, TILE), jnp.float32) ** steps_of(keys[3], (N_PX, N_PY * TILES_DEV, TILE), ((0, 8), (1, 4)), -0.2, 0.2)), 0.25, 4.0).astype(jnp.bfloat16),
        "live": draw_live(jax.random.fold_in(keys[7], 71), 0),
        "tile_owner": draw_tile_owner(jax.random.fold_in(keys[7], 71), 0),
        "counts": draw_counts(jax.random.fold_in(keys[7], 71), 0),
    }


BETA = 18.4

def kernel(spread_at):
    return jnp.exp(BETA * (jnp.sqrt(1.0 - spread_at * spread_at) - 1.0))

def reference(cell_ids, offset_x, offset_y, mass, live, tile_owner, counts):
    tile_shape = (N_PX, N_PY, TILES_DEV, TILE)
    tile_cells = cell_ids.reshape(tile_shape)
    frac_x = offset_x.reshape(tile_shape).astype(jnp.float32)
    frac_y = offset_y.reshape(tile_shape).astype(jnp.float32)
    masses = jnp.where(live == 1, mass, jnp.zeros_like(mass)).reshape(tile_shape).astype(jnp.float32)
    owners = tile_owner.reshape(N_PX, N_PY, TILES_DEV)
    offset_steps = jnp.arange(-3, 5, dtype=jnp.int32)
    step_values = offset_steps.astype(jnp.float32)
    column_base = (jnp.arange(N_PY, dtype=jnp.int32) * RY)[:, None, None]

    def deposit_rows(density_flat, source_rows):
        row_cells, row_x, row_y, row_mass, row_owner = source_rows
        local_y = row_cells % RY
        local_x = row_cells // RY % RX
        plane_ids = row_cells // (RY * RX)
        global_x = row_owner[:, :, None] * RX + local_x
        global_y = column_base + local_y
        weight_x = kernel((step_values - row_x[..., None]) / 4.0).astype(jnp.bfloat16)
        weight_y = (kernel((step_values - row_y[..., None]) / 4.0) * row_mass[..., None]).astype(jnp.bfloat16)
        weight_x, weight_y = lax.optimization_barrier((weight_x, weight_y))
        values = weight_x.astype(jnp.float32)[..., :, None] * weight_y.astype(jnp.float32)[..., None, :]
        rows_at = (global_x[..., None] + offset_steps) % NX
        columns_at = (global_y[..., None] + offset_steps) % NY
        flat_index = (plane_ids[..., None, None] * NX + rows_at[..., :, None]) * NY + columns_at[..., None, :]
        return (density_flat.at[flat_index.reshape(-1)].add(values.reshape(-1)), None)
    initial = jnp.zeros((PLANES * NX * NY,), jnp.float32)
    density_flat = lax.scan(deposit_rows, initial, (tile_cells, frac_x, frac_y, masses, owners))[0]
    density = density_flat.reshape(PLANES, NX, NY)
    mean_density = jnp.sum(density) / (PLANES * NX * NY)
    contrast = density / mean_density - 1.0
    transform = jnp.fft.fft2(contrast, axes=(1, 2)) / math.sqrt(NX * NY)
    transform = jnp.transpose(transform, (0, 2, 1))
    spectrum = jnp.stack([jnp.real(transform), jnp.imag(transform)]).astype(jnp.float32)
    column_totals = lax.optimization_barrier(jnp.sum(counts, axis=0))
    preceding = jnp.cumsum(column_totals, axis=-1) - column_totals
    earlier = jnp.cumsum(counts, axis=0) - counts
    bucket_start = (preceding[None] + earlier).astype(jnp.int32)
    return (spectrum, bucket_start)
```

```python
import functools
import math

import jax
import jax.numpy as jnp
import numpy as np
from jax import lax
from jax.experimental import pallas as pl
from jax.experimental.pallas import tpu as pltpu
from jax.sharding import PartitionSpec as P

NX = 1024
NY = 1024
PLANES = 8
BETA = 18.4
LANES = 128
GROUP = 4


def tap_blocks(start, fraction, scaling):
    rows = lax.broadcasted_iota(jnp.int32, (8, LANES), 0)
    first = jnp.broadcast_to(start, (8, LANES)) - 3
    depth = (rows - first) & 7
    z = ((depth - 3).astype(jnp.float32) - fraction) * 0.25
    taps = jnp.exp(BETA * (jnp.sqrt(jnp.maximum(1.0 - z * z, 0.0)) - 1.0))
    if scaling is not None:
        taps = taps * scaling
    block = (first + depth) >> 3
    odd = (block & 1) == 1
    zero = jnp.zeros_like(taps)
    both = jnp.concatenate(
        [jnp.where(odd, zero, taps), jnp.where(odd, taps, zero)], axis=0
    ).astype(jnp.bfloat16)
    half = block >> 1
    return both, half


def spread_kernel(row_count, col_count, bucket_count, starts_ref, lx_ref, ly_ref, fx_ref, fy_ref,
                  w_ref, out_ref, acc_ref, wx_ref, wy_ref):
    col_blocks = col_count // 16
    lane_tiles = NX // LANES
    out_ref[...] = jnp.zeros_like(out_ref)
    wx_ref[...] = jnp.zeros_like(wx_ref)
    height = col_count + 16
    lane = lax.broadcasted_iota(jnp.int32, (height, LANES), 1)

    def bucket(b, _):
        begin = starts_ref[b]
        end = starts_ref[b + 1]
        chunks = (end - begin + GROUP - 1) // GROUP

        @pl.when(chunks > 0)
        def _():
            acc_ref[...] = jnp.zeros_like(acc_ref)

            def chunk(c, _):
                for g in range(GROUP):
                    t = begin + c * GROUP + g
                    at = pl.ds(t, 1)
                    scale = jnp.where(t < end, 1.0, 0.0)
                    taps, block = tap_blocks(lx_ref[at, :], fx_ref[at, :], None)
                    block = jnp.concatenate([block, block], axis=0).astype(jnp.int16)
                    none = jnp.zeros_like(taps)
                    cols = pl.ds(g * LANES, LANES)
                    for k in range(9):
                        wx_ref[pl.ds(k * 16, 16), cols] = jnp.where(block == k, taps, none)
                    wx_ref[pl.ds(240, 16), cols] = jnp.where(block == -1, taps, none)
                    taps, block = tap_blocks(ly_ref[at, :], fy_ref[at, :], w_ref[at, :] * scale)
                    block = jnp.where(block < 0, col_blocks, block)
                    block = jnp.concatenate([block, block], axis=0).astype(jnp.int16)
                    for k in range(col_blocks + 1):
                        wy_ref[pl.ds(k * 16, 16), cols] = jnp.where(block == k, taps, none)
                acc_ref[...] += lax.dot_general(
                    wy_ref[...], wx_ref[...], (((1,), (1,)), ((), ())),
                    preferred_element_type=jnp.float32,
                )
                return 0

            lax.fori_loop(0, chunks, chunk, 0)
            plane = b % PLANES
            tile = (b // PLANES * row_count) // LANES
            here = pl.ds(pl.multiple_of(tile * LANES, LANES), LANES)
            after = pl.ds(pl.multiple_of((tile + 1) % lane_tiles * LANES, LANES), LANES)
            before = pl.ds(pl.multiple_of((tile + lane_tiles - 1) % lane_tiles * LANES, LANES), LANES)
            out_ref[plane, :, here] += acc_ref[:, :LANES]
            rim = acc_ref[:, LANES:]
            out_ref[plane, :, after] += jnp.where(lane < 64, rim, 0.0)
            out_ref[plane, :, before] += jnp.where(lane < 64, 0.0, rim)
        return 0

    lax.fori_loop(0, bucket_count, bucket, 0)


def spread(starts, lx, ly, fx, fy, w, row_count, col_count):
    height = col_count + 16
    bucket_count = starts.shape[0] - 1
    vmem = pl.BlockSpec(memory_space=pltpu.VMEM)
    return pl.pallas_call(
        functools.partial(spread_kernel, row_count, col_count, bucket_count),
        out_shape=jax.ShapeDtypeStruct((PLANES, height, NX), jnp.float32),
        in_specs=[pl.BlockSpec(memory_space=pltpu.SMEM)] + [vmem] * 5,
        out_specs=vmem,
        scratch_shapes=[
            pltpu.VMEM((height, 2 * LANES), jnp.float32),
            pltpu.VMEM((2 * LANES, GROUP * LANES), jnp.bfloat16),
            pltpu.VMEM((height, GROUP * LANES), jnp.bfloat16),
        ],
        compiler_params=pltpu.CompilerParams(vmem_limit_bytes=40 * 1024 * 1024),
        name="spread",
    )(starts, lx, ly, fx, fy, w)


def split(value):
    high = lax.reduce_precision(value, 8, 7)
    return high.astype(jnp.bfloat16), (value - high).astype(jnp.bfloat16)


def dft_tables():
    n = np.arange(NX)
    k = np.arange(32)
    coarse = 2.0 * np.pi / NX * ((32 * k[:, None] * n[None, :]) % NX)
    fine = 2.0 * np.pi / NX * ((k[:, None] * n[None, :]) % NX)
    cc, cs, fc, fs = lax.optimization_barrier(
        tuple(jnp.asarray(f(a), jnp.float32) for a in (coarse, fine) for f in (np.cos, np.sin))
    )
    cc, cs = cc[:, None, :], cs[:, None, :]
    fc, fs = fc[None, :, :], fs[None, :, :]
    cosine = (cc * fc - cs * fs).reshape(NX, NX)
    sine = (cs * fc + cc * fs).reshape(NX, NX)
    return split(cosine) + split(sine)


def dot(a, b):
    return jnp.dot(a, b, preferred_element_type=jnp.float32)


def local(cell_ids, offset_x, offset_y, mass, live, tile_owner, counts):
    px_count = lax.axis_size("px")
    py_count = lax.axis_size("py")
    row_count = NX // px_count
    col_count = NY // py_count
    parts = px_count // PLANES
    cells = cell_ids[0]
    owners = tile_owner[0]
    buckets = owners * PLANES + cells[:, 0] // (row_count * col_count)
    edges = jnp.arange(px_count * PLANES + 1, dtype=jnp.int32)
    starts = jnp.sum((buckets[None, :] < edges[:, None]).astype(jnp.int32), axis=1)

    def padded(value):
        return jnp.pad(value, ((0, 8), (0, 0)))

    ly = padded(cells % col_count)
    lx = padded((cells // col_count % row_count + owners[:, None] * row_count) % LANES)
    fx = padded(offset_x[0].astype(jnp.float32))
    fy = padded(offset_y[0].astype(jnp.float32))
    w = padded(jnp.where(live[0] == 1, mass[0], jnp.zeros_like(mass[0])).astype(jnp.float32))
    grid = spread(starts, lx, ly, fx, fy, w, row_count, col_count)
    height = col_count + 16
    width = NX // parts
    if parts > 1:
        grid = grid.reshape(PLANES, height, parts, width).transpose(0, 2, 1, 3)
        grid = grid.reshape(px_count, height, width)
    mine = lax.psum_scatter(grid, "px", scatter_dimension=0, tiled=True)[0]
    total = lax.psum(jnp.sum(mine), ("px", "py"))
    by_cols = lax.all_to_all(mine, "py", split_axis=1, concat_axis=0, tiled=True)
    part = width // py_count
    ext = by_cols.reshape(py_count, height, part)
    core = ext[:, :col_count]
    right = jnp.roll(ext[:, col_count : col_count + 4], 1, axis=0)
    left = jnp.roll(ext[:, col_count + 12 :], -1, axis=0)
    core = core + jnp.concatenate(
        [right, jnp.zeros((py_count, col_count - 8, part), jnp.float32), left], axis=1
    )
    data = core.reshape(NY, part)
    cos_hi, cos_lo, sin_hi, sin_lo = dft_tables()
    hi, lo = split(data)
    both = jnp.concatenate([hi, lo], axis=1)
    real = dot(cos_hi, both)
    real = real[:, :part] + real[:, part:] + dot(cos_lo, hi)
    imag = dot(sin_hi, both)
    imag = -(imag[:, :part] + imag[:, part:] + dot(sin_lo, hi))
    devices = px_count * py_count
    ky_part = NY // devices
    lines = jnp.stack([real, imag]).reshape(2, devices, ky_part, part).transpose(1, 0, 2, 3)
    got = lax.all_to_all(lines, ("px", "py"), split_axis=0, concat_axis=0, tiled=True)
    got = got.reshape(PLANES, parts * py_count, 2, ky_part, part).transpose(2, 0, 3, 1, 4)
    got = got.reshape(2 * PLANES * ky_part, NX)
    hi, lo = split(got)
    rows = PLANES * ky_part
    both = jnp.concatenate([hi, lo], axis=0)
    by_cos = dot(both, cos_hi)
    by_cos = by_cos[: 2 * rows] + by_cos[2 * rows :] + dot(hi, cos_lo)
    by_sin = dot(both, sin_hi)
    by_sin = by_sin[: 2 * rows] + by_sin[2 * rows :] + dot(hi, sin_lo)
    out = jnp.stack([by_cos[:rows] + by_sin[rows:], by_cos[rows:] - by_sin[:rows]])
    out = out.reshape(2, PLANES, ky_part, NX)
    norm = 1.0 / math.sqrt(NX * NY)
    index = lax.axis_index("px") * py_count + lax.axis_index("py")
    shape = (2, 1, ky_part, NX)
    at_zero = (
        (lax.broadcasted_iota(jnp.int32, shape, 0) == 0)
        & (lax.broadcasted_iota(jnp.int32, shape, 2) + index == 0)
        & (lax.broadcasted_iota(jnp.int32, shape, 3) == 0)
    )
    spectrum = out * (PLANES * NX * NY * norm / total) - jnp.where(at_zero, NX * NY * norm, 0.0)
    column = lax.all_gather(counts, "px")
    column_sum = jnp.sum(column, axis=0)
    reached = lax.broadcasted_iota(jnp.int32, column.shape, 0) < lax.axis_index("px")
    earlier = jnp.sum(jnp.where(reached, column, 0), axis=0)
    preceding = jnp.cumsum(column_sum, axis=-1) - column_sum
    bucket_start = (preceding + earlier).astype(jnp.int32)
    return (spectrum, bucket_start)


def solution(mesh):
    placed = (
        P("px", "py", None),
        P("px", "py", None),
        P("px", "py", None),
        P("px", "py", None),
        P("px", "py", None),
        P("px", "py"),
        P("px", "py", None),
    )
    return jax.shard_map(
        local,
        mesh=mesh,
        in_specs=placed,
        out_specs=(P(None, None, ("px", "py"), None), P("px", "py", None)),
        check_vma=False,
    )
```

```python
import functools
import math

import jax
import jax.numpy as jnp
import numpy as np
from jax import lax
from jax.experimental import pallas as pl
from jax.experimental.pallas import tpu as pltpu
from jax.sharding import PartitionSpec as P

NX = 1024
NY = 1024
PLANES = 8
BETA = 18.4
LANES = 128
GROUP = 4


def tap_blocks(start, fraction, scaling):
    rows = lax.broadcasted_iota(jnp.int32, (8, LANES), 0)
    first = jnp.broadcast_to(start, (8, LANES)) - 3
    depth = (rows - first) & 7
    z = ((depth - 3).astype(jnp.float32) - fraction) * 0.25
    taps = jnp.exp(BETA * (jnp.sqrt(jnp.maximum(1.0 - z * z, 0.0)) - 1.0))
    if scaling is not None:
        taps = taps * scaling
    block = (first + depth) >> 3
    odd = (block & 1) == 1
    zero = jnp.zeros_like(taps)
    both = jnp.concatenate(
        [jnp.where(odd, zero, taps), jnp.where(odd, taps, zero)], axis=0
    ).astype(jnp.bfloat16)
    half = block >> 1
    return both, half


def spread_kernel(row_count, col_count, bucket_count, starts_ref, lx_ref, ly_ref, fx_ref, fy_ref,
                  w_ref, out_ref, acc_ref, wx_ref, wy_ref):
    col_blocks = col_count // 16
    lane_tiles = NX // LANES
    out_ref[...] = jnp.zeros_like(out_ref)
    wx_ref[...] = jnp.zeros_like(wx_ref)
    height = col_count + 16
    lane = lax.broadcasted_iota(jnp.int32, (height, LANES), 1)

    def bucket(b, _):
        begin = starts_ref[b]
        end = starts_ref[b + 1]
        chunks = (end - begin + GROUP - 1) // GROUP

        @pl.when(chunks > 0)
        def _():
            acc_ref[...] = jnp.zeros_like(acc_ref)

            def chunk(c, _):
                for g in range(GROUP):
                    t = begin + c * GROUP + g
                    at = pl.ds(t, 1)
                    scale = jnp.where(t < end, 1.0, 0.0)
                    taps, block = tap_blocks(lx_ref[at, :], fx_ref[at, :], None)
                    block = jnp.concatenate([block, block], axis=0).astype(jnp.int16)
                    none = jnp.zeros_like(taps)
                    cols = pl.ds(g * LANES, LANES)
                    for k in range(9):
                        wx_ref[pl.ds(k * 16, 16), cols] = jnp.where(block == k, taps, none)
                    wx_ref[pl.ds(240, 16), cols] = jnp.where(block == -1, taps, none)
                    taps, block = tap_blocks(ly_ref[at, :], fy_ref[at, :], w_ref[at, :] * scale)
                    block = jnp.where(block < 0, col_blocks, block)
                    block = jnp.concatenate([block, block], axis=0).astype(jnp.int16)
                    for k in range(col_blocks + 1):
                        wy_ref[pl.ds(k * 16, 16), cols] = jnp.where(block == k, taps, none)
                acc_ref[...] += lax.dot_general(
                    wy_ref[...], wx_ref[...], (((1,), (1,)), ((), ())),
                    preferred_element_type=jnp.float32,
                )
                return 0

            lax.fori_loop(0, chunks, chunk, 0)
            plane = b % PLANES
            tile = (b // PLANES * row_count) // LANES
            here = pl.ds(pl.multiple_of(tile * LANES, LANES), LANES)
            after = pl.ds(pl.multiple_of((tile + 1) % lane_tiles * LANES, LANES), LANES)
            before = pl.ds(pl.multiple_of((tile + lane_tiles - 1) % lane_tiles * LANES, LANES), LANES)
            out_ref[plane, :, here] += acc_ref[:, :LANES]
            rim = acc_ref[:, LANES:]
            out_ref[plane, :, after] += jnp.where(lane < 64, rim, 0.0)
            out_ref[plane, :, before] += jnp.where(lane < 64, 0.0, rim)
        return 0

    lax.fori_loop(0, bucket_count, bucket, 0)


def spread(starts, lx, ly, fx, fy, w, row_count, col_count):
    height = col_count + 16
    bucket_count = starts.shape[0] - 1
    vmem = pl.BlockSpec(memory_space=pltpu.VMEM)
    return pl.pallas_call(
        functools.partial(spread_kernel, row_count, col_count, bucket_count),
        out_shape=jax.ShapeDtypeStruct((PLANES, height, NX), jnp.float32),
        in_specs=[pl.BlockSpec(memory_space=pltpu.SMEM)] + [vmem] * 5,
        out_specs=vmem,
        scratch_shapes=[
            pltpu.VMEM((height, 2 * LANES), jnp.float32),
            pltpu.VMEM((2 * LANES, GROUP * LANES), jnp.bfloat16),
            pltpu.VMEM((height, GROUP * LANES), jnp.bfloat16),
        ],
        compiler_params=pltpu.CompilerParams(vmem_limit_bytes=40 * 1024 * 1024),
        name="spread",
    )(starts, lx, ly, fx, fy, w)


def split(value):
    high = lax.reduce_precision(value, 8, 7)
    return high.astype(jnp.bfloat16), (value - high).astype(jnp.bfloat16)


def dft_tables():
    n = np.arange(NX)
    k = np.arange(32)
    coarse = 2.0 * np.pi / NX * ((32 * k[:, None] * n[None, :]) % NX)
    fine = 2.0 * np.pi / NX * ((k[:, None] * n[None, :]) % NX)
    cc, cs, fc, fs = lax.optimization_barrier(
        tuple(jnp.asarray(f(a), jnp.float32) for a in (coarse, fine) for f in (np.cos, np.sin))
    )
    cc, cs = cc[:, None, :], cs[:, None, :]
    fc, fs = fc[None, :, :], fs[None, :, :]
    cosine = (cc * fc - cs * fs).reshape(NX, NX)
    sine = (cs * fc + cc * fs).reshape(NX, NX)
    return split(cosine) + split(sine)


def dot(a, b):
    return jnp.dot(a, b, preferred_element_type=jnp.float32)


def power_of(top):
    return jnp.clip(jnp.floor(jnp.log2(jnp.maximum(top, 1e-30))) + 1.0, -90.0, 90.0).astype(jnp.int32)


def scale_of(power):
    return jnp.exp2((power - 15).astype(jnp.float32))


def coded_as(value, power):
    steps = jnp.round(value * jnp.exp2((15 - power).astype(jnp.float32)))
    return jnp.clip(steps, -32767.0, 32767.0).astype(jnp.int16)


def coded_rows(value, spare):
    power = power_of(jnp.max(jnp.abs(value), axis=-2, keepdims=True))
    row = lax.broadcasted_iota(jnp.int32, value.shape, value.ndim - 2)
    return jnp.where(row == spare, power.astype(jnp.int16), coded_as(value, power))


def plain_rows(coded, spare):
    power = lax.slice_in_dim(coded, spare, spare + 1, axis=coded.ndim - 2).astype(jnp.int32)
    row = lax.broadcasted_iota(jnp.int32, coded.shape, coded.ndim - 2)
    return jnp.where(row == spare, 0.0, coded.astype(jnp.float32) * scale_of(power))


def digits(value, width):
    power = power_of(value)
    scaled = value * jnp.exp2((14 - power).astype(jnp.float32))
    high = jnp.clip(jnp.floor(scaled), 0.0, 32767.0)
    low = jnp.clip(jnp.floor((scaled - high) * 16384.0), 0.0, 16384.0)
    lane = lax.broadcasted_iota(jnp.int32, (1, width), 1)
    rest = jnp.where(lane == 1, high, low).astype(jnp.int32)
    return jnp.where(lane == 0, power, rest)


def number(row):
    value = row[..., 1].astype(jnp.float32) + row[..., 2].astype(jnp.float32) / 16384.0
    return value * jnp.exp2((row[..., 0] - 14).astype(jnp.float32))


def local(cell_ids, offset_x, offset_y, mass, live, tile_owner, counts):
    px_count = lax.axis_size("px")
    py_count = lax.axis_size("py")
    row_count = NX // px_count
    col_count = NY // py_count
    parts = px_count // PLANES
    cells = cell_ids[0]
    owners = tile_owner[0]
    buckets = owners * PLANES + cells[:, 0] // (row_count * col_count)
    edges = jnp.arange(px_count * PLANES + 1, dtype=jnp.int32)
    starts = jnp.sum((buckets[None, :] < edges[:, None]).astype(jnp.int32), axis=1)

    def padded(value):
        return jnp.pad(value, ((0, 8), (0, 0)))

    ly = padded(cells % col_count)
    lx = padded((cells // col_count % row_count + owners[:, None] * row_count) % LANES)
    fx = padded(offset_x[0].astype(jnp.float32))
    fy = padded(offset_y[0].astype(jnp.float32))
    w = padded(jnp.where(live[0] == 1, mass[0], jnp.zeros_like(mass[0])).astype(jnp.float32))
    grid = spread(starts, lx, ly, fx, fy, w, row_count, col_count)
    height = col_count + 16
    width = NX // parts
    if parts > 1:
        grid = grid.reshape(PLANES, height, parts, width).transpose(0, 2, 1, 3)
    grid = grid.reshape(px_count // 2, 2, height, width)
    side = lax.axis_index("px") % 2
    keep = lax.dynamic_index_in_dim(grid, side, 1, keepdims=False)
    away = lax.dynamic_index_in_dim(grid, 1 - side, 1, keepdims=False)
    pairs = [(source, source ^ 1) for source in range(px_count)]
    summed = keep + lax.ppermute(away, "px", pairs)
    groups = [list(range(k, px_count, 2)) for k in range(2)]
    got = lax.all_to_all(
        coded_rows(summed, col_count + 8), "px", 0, 0, axis_index_groups=groups, tiled=True
    )
    mine = jnp.sum(plain_rows(got, col_count + 8), axis=0)
    total = jnp.sum(mine)
    by_cols = lax.all_to_all(
        coded_rows(mine, col_count + 8), "py", split_axis=1, concat_axis=0, tiled=True
    )
    part = width // py_count
    ext = plain_rows(by_cols.reshape(py_count, height, part), col_count + 8)
    core = ext[:, :col_count]
    right = jnp.roll(ext[:, col_count : col_count + 4], 1, axis=0)
    left = jnp.roll(ext[:, col_count + 12 :], -1, axis=0)
    core = core + jnp.concatenate(
        [right, jnp.zeros((py_count, col_count - 8, part), jnp.float32), left], axis=1
    )
    data = core.reshape(NY, part)
    cos_hi, cos_lo, sin_hi, sin_lo = dft_tables()
    hi, lo = split(data)
    both = jnp.concatenate([hi, lo], axis=1)
    real = dot(cos_hi, both)
    real = real[:, :part] + real[:, part:] + dot(cos_lo, hi)
    imag = dot(sin_hi, both)
    imag = -(imag[:, :part] + imag[:, part:] + dot(sin_lo, hi))
    devices = px_count * py_count
    ky_part = NY // devices
    lines = jnp.stack([real.reshape(devices, ky_part, part), imag.reshape(devices, ky_part, part)], 1)
    lines = lines.reshape(devices, 2 * ky_part, part)
    power = power_of(jnp.max(jnp.abs(lines), axis=1, keepdims=True))
    coded = coded_as(lines, power)
    bucket_count = counts.shape[-1]
    count_rows = -(-bucket_count // part)
    spare = -(2 + count_rows) % 8
    side_rows = jnp.concatenate(
        [
            digits(total, part),
            jnp.pad(counts.reshape(-1), (0, count_rows * part - bucket_count)).reshape(-1, part),
            jnp.zeros((spare, part), jnp.int32),
        ]
    ).astype(jnp.int16)
    side_rows = jnp.broadcast_to(side_rows[None], (devices,) + side_rows.shape)
    coded = jnp.concatenate([coded, power.astype(jnp.int16), side_rows], axis=1)
    got = lax.all_to_all(coded, ("px", "py"), split_axis=0, concat_axis=0, tiled=True)
    after = got[:, 2 * ky_part :].astype(jnp.int32)
    lines = got[:, : 2 * ky_part].astype(jnp.float32) * scale_of(after[:, :1])
    total = jnp.sum(number(after[:, 1]))
    column = after[:, 2 : 2 + count_rows].reshape(px_count, py_count, 1, count_rows * part)
    column = lax.dynamic_index_in_dim(column, lax.axis_index("py"), 1, keepdims=False)
    column = column[:, :, :bucket_count][:, None]
    got = lines.reshape(PLANES, parts * py_count, 2, ky_part, part).transpose(2, 0, 3, 1, 4)
    got = got.reshape(2 * PLANES * ky_part, NX)
    hi, lo = split(got)
    rows = PLANES * ky_part
    both = jnp.concatenate([hi, lo], axis=0)
    by_cos = dot(both, cos_hi)
    by_cos = by_cos[: 2 * rows] + by_cos[2 * rows :] + dot(hi, cos_lo)
    by_sin = dot(both, sin_hi)
    by_sin = by_sin[: 2 * rows] + by_sin[2 * rows :] + dot(hi, sin_lo)
    out = jnp.stack([by_cos[:rows] + by_sin[rows:], by_cos[rows:] - by_sin[:rows]])
    out = out.reshape(2, PLANES, ky_part, NX)
    norm = 1.0 / math.sqrt(NX * NY)
    index = lax.axis_index("px") * py_count + lax.axis_index("py")
    shape = (2, 1, ky_part, NX)
    at_zero = (
        (lax.broadcasted_iota(jnp.int32, shape, 0) == 0)
        & (lax.broadcasted_iota(jnp.int32, shape, 2) + index == 0)
        & (lax.broadcasted_iota(jnp.int32, shape, 3) == 0)
    )
    spectrum = out * (PLANES * NX * NY * norm / total) - jnp.where(at_zero, NX * NY * norm, 0.0)
    column_sum = jnp.sum(column, axis=0)
    reached = lax.broadcasted_iota(jnp.int32, column.shape, 0) < lax.axis_index("px")
    earlier = jnp.sum(jnp.where(reached, column, 0), axis=0)
    preceding = jnp.cumsum(column_sum, axis=-1) - column_sum
    bucket_start = (preceding + earlier).astype(jnp.int32)
    return (spectrum, bucket_start)


def solution(mesh):
    placed = (
        P("px", "py", None),
        P("px", "py", None),
        P("px", "py", None),
        P("px", "py", None),
        P("px", "py", None),
        P("px", "py"),
        P("px", "py", None),
    )
    return jax.shard_map(
        local,
        mesh=mesh,
        in_specs=placed,
        out_specs=(P(None, None, ("px", "py"), None), P("px", "py", None)),
        check_vma=False,
    )
```
